32 devices in a mesh: rows: 4 (over z), snaps: 8 (over y, x, core).
Axes of the slice: x: 2, y: 2, z: 4, core: 2. Of those that a mesh axis runs over, the one named last changes fastest.
Arguments:
- snapshots: float32 [8192, 2048], P('rows', 'snaps'), may hold values from -6 to 6
- weights: float32 [8192], P('rows'), may hold values from 0.3 to 3
- next_bricks: float32 [8192, 2048], P(('rows', 'snaps')), may hold values from -6 to 6
- brick_source: int32 [4, 64], P('rows'), may hold values from 0 to 63, each once within a row
Outputs:
- gram: float32 [2048, 2048], P('rows', 'snaps')
- next_tiles: float32 [8192, 2048], P('rows', 'snaps')
The draws below stay inside these ranges and needn't reach their ends.
Inputs may be any that keep to these rules, and one draw needn't show every extreme that they name: Each row of brick_source is a permutation of 0 to 63.
All inputs are finite; a program needn't handle non-finite values.
Results may differ from the reference program's by a relative error of at most 0.00007.
Values sent between devices are 32-bit elements; how exact they have to be, the bound alone decides.
A program may use at most 128 MiB of HBM per device.

```python
import math
import jax
import jax.numpy as jnp
from jax import lax

BRICK = 32
S = 2048
M = 8192
BRICKS_DEV = 64
N_ROWS = 4


def level_of(stream_key, extent, shards, low, high):
    factor_of = 1.0
    for position, parts in shards:
        heights = jax.random.uniform(jax.random.fold_in(jax.random.fold_in(stream_key, 6), position), (parts,), jnp.float32, low / len(shards), high / len(shards))
        factor_of = factor_of * jnp.repeat(jnp.exp(heights), extent[position] // parts).reshape((-1,) + (1,) * (len(extent) - 1 - position))
    return factor_of


def normal_values(stream_key, dims, scale, reach, pieces=(), dtype=jnp.bfloat16):
    result = jax.random.normal(stream_key, dims, jnp.float32) * scale
    if len(pieces) > 0:
        result = level_of(stream_key, dims, pieces, -0.22, 0.18) * result
    return jnp.clip(result, min=-reach, max=reach).astype(dtype)


def setup_inputs(seed: int = 0) -> dict:
    key_of = jax.random.split(jax.random.key(seed), 5)
    snapshots = normal_values(key_of[0], (M, S), 1.0, 6.0, ((0, 4), (1, 8)), jnp.float32)
    weights = jnp.clip(jnp.exp(math.log(3.0) - 2.3025851 * jax.random.uniform(key_of[1], (M,), jnp.float32) ** level_of(key_of[1], (M,), ((0, 4),), -0.2, 0.2)), 0.3, 3.0)
    next_bricks = normal_values(key_of[2], (M, S), 1.0, 6.0, ((0, 32),), jnp.float32)
    brick_source = jax.vmap(lambda own: jax.random.permutation(own, BRICKS_DEV))(jax.random.split(key_of[3], N_ROWS)).reshape((N_ROWS, BRICKS_DEV)).astype(jnp.int32)
    return dict(snapshots=snapshots, weights=weights, next_bricks=next_bricks, brick_source=brick_source)


def pick_bricks(block, order):
    return jnp.take(block, order, axis=0)

def reference(snapshots, weights, next_bricks, brick_source):
    weighted = snapshots * weights[:, None]
    product = lax.dot_general(snapshots, weighted, (((0,), (0,)), ((), ())), precision=lax.Precision.HIGHEST, preferred_element_type=jnp.float32)
    gram = product / jnp.float32(math.sqrt(M))
    blocks = next_bricks.reshape(N_ROWS, BRICKS_DEV, BRICK, S)
    moved = jax.vmap(pick_bricks)(blocks, brick_source)
    next_tiles = moved.reshape(M, S)
    return (gram, next_tiles)
```

```python
import functools
import math

import jax
import jax.numpy as jnp
from jax import lax
from jax.experimental import pallas as pl
from jax.experimental.pallas import tpu as pltpu
from jax.sharding import PartitionSpec as P

MESH = pl.DeviceIdType.MESH
STEP = 256
PIECES = 2
GROUPS = 8


def split(x):
    hi = x.astype(jnp.bfloat16)
    return hi, (x - hi.astype(jnp.float32)).astype(jnp.bfloat16)


def tdot(a, b):
    return lax.dot_general(a, b, (((0,), (0,)), ((), ())), preferred_element_type=jnp.float32)


def kernel(
    n_r, n_s, scale,
    snap, wts, bricks,
    gram, arrived,
    gbuf, mate, w_hi, w_lo, part, rs_buf, h_send, h_recv,
    ring_send, ring_recv, brick_send, brick_recv, rs_send, rs_recv, d_send, d_recv, own_sem,
):
    n = n_s // 2
    z = lax.axis_index("rows")
    s = lax.axis_index("snaps")
    c = s % 2
    chip = s // 2
    rows, width = snap.shape
    per_brick_dev = bricks.shape[0]

    def ring_of(i):
        u, v = i // 2, i % 2
        return u + v * (n - 1 - 2 * u)

    def chip_at(t):
        v = t // (n // 2)
        return 2 * (t + v * (n - 1 - 2 * t)) + v

    t = ring_of(chip)
    partner = chip * 2 + (1 - c)
    nxt = chip_at((t + 1) % n) * 2 + c
    prv = chip_at((t + n - 1) % n) * 2 + c

    barrier = pltpu.get_barrier_semaphore()
    for k in range(1, n_s):
        pl.semaphore_signal(barrier, inc=1, device_id=(z, (s + k) % n_s), device_id_type=MESH)
    for k in range(1, n_r):
        pl.semaphore_signal(barrier, inc=1, device_id=((z + k) % n_r, s), device_id_type=MESH)
    pl.semaphore_wait(barrier, n_s - 1 + n_r - 1)

    half = rows // 2
    piece = half // PIECES

    def ring_copy(way, hop, q):
        r0 = way * half + q * piece
        there = (n - hop if way == 0 else hop) - 1
        if hop == 1:
            src = snap.at[pl.ds(r0, piece)]
        else:
            here = (n - hop + 1 if way == 0 else hop - 1) - 1
            src = gbuf.at[here, pl.ds(r0, piece)]
        return pltpu.make_async_remote_copy(
            src_ref=src,
            dst_ref=gbuf.at[there, pl.ds(r0, piece)],
            send_sem=ring_send.at[way, hop - 1, q],
            recv_sem=ring_recv.at[way, hop - 1, q],
            device_id=(z, nxt if way == 0 else prv),
            device_id_type=MESH,
        )

    def brick_copy(k):
        to = (s + k) % n_s
        return pltpu.make_async_remote_copy(
            src_ref=bricks.at[:, pl.ds(pl.multiple_of(to * width, width), width)],
            dst_ref=arrived.at[pl.ds(pl.multiple_of(s * per_brick_dev, per_brick_dev), per_brick_dev)],
            send_sem=brick_send.at[k - 1],
            recv_sem=brick_recv.at[k - 1],
            device_id=(z, to),
            device_id_type=MESH,
        )

    def rs_copy(slot, k, home):
        return pltpu.make_async_remote_copy(
            src_ref=part.at[slot],
            dst_ref=rs_buf.at[k - 1],
            send_sem=rs_send.at[k - 1],
            recv_sem=rs_recv.at[k - 1],
            device_id=(home, s),
            device_id_type=MESH,
        )

    def d2d(i, src, dst):
        return pltpu.make_async_remote_copy(
            src_ref=src, dst_ref=dst, send_sem=d_send.at[i], recv_sem=d_recv.at[i],
            device_id=(z, partner), device_id_type=MESH,
        )

    for q in range(PIECES):
        for way in range(2):
            ring_copy(way, 1, q).start()
    own_bricks = pltpu.make_async_copy(
        bricks.at[:, pl.ds(pl.multiple_of(s * width, width), width)],
        arrived.at[pl.ds(pl.multiple_of(s * per_brick_dev, per_brick_dev), per_brick_dev)],
        own_sem.at[0],
    )
    own_bricks.start()
    to_mate = d2d(0, snap, mate)
    to_mate.start()

    def weigh(src, col):
        def body(i, carry):
            r0 = pl.multiple_of(i * 128, 128)
            w = jnp.broadcast_to(wts[pl.ds(i, 1), :], (128, 128)).T
            for l in range(width // 128):
                hi, lo = split(src[pl.ds(r0, 128), l * 128:(l + 1) * 128] * w)
                w_hi[pl.ds(r0, 128), col + l * 128:col + (l + 1) * 128] = hi
                w_lo[pl.ds(r0, 128), col + l * 128:col + (l + 1) * 128] = lo
            return carry
        lax.fori_loop(0, rows // 128, body, 0)

    def gather_product(slot, load, r0, count):
        def body(i, carry):
            r = pl.multiple_of(r0 + i * STEP, STEP)
            hi, lo = split(load(r))
            bh = w_hi[pl.ds(r, STEP), :]
            bl = w_lo[pl.ds(r, STEP), :]
            part[slot] += tdot(hi, bh) + (tdot(hi, bl) + tdot(lo, bh))
            return carry
        lax.fori_loop(0, count // STEP, body, 0)

    def send_home(slot):
        home = chip_at((t + slot) % n)
        k = (home + n_r - z) % n_r

        @pl.when(k > 0)
        def _():
            rs_copy(slot, k, home).start()

    weigh(snap, 0)
    part[...] = jnp.zeros_like(part)
    to_mate.wait()
    weigh(mate, width)
    gather_product(0, lambda r: snap[pl.ds(r, STEP), :], 0, rows)
    send_home(0)

    done = [0] * n
    for hop in range(1, n):
        for q in range(PIECES):
            for way in range(2):
                ring_copy(way, hop, q).wait_recv()
                if hop < n - 1:
                    ring_copy(way, hop + 1, q).start()
            if q == PIECES - 1 and hop == n - 2:
                for k in range(1, n_s):
                    brick_copy(k).start()
            for way in range(2):
                slot = n - hop if way == 0 else hop
                gather_product(
                    slot,
                    lambda r, slot=slot: gbuf[slot - 1, pl.ds(r, STEP), :],
                    way * half + q * piece,
                    piece,
                )
        for way in range(2):
            slot = n - hop if way == 0 else hop
            done[slot] += 1
            if done[slot] == 2:
                send_home(slot)

    for k in range(1, n_r):
        rs_copy(0, k, (z + k) % n_r).wait_recv()
    own = (ring_of(z) + n - t) % n
    total = part[own]
    for k in range(1, n_r):
        total += rs_buf[k - 1]
    total = total / scale
    h_send[...] = total[:, width:]
    to_other = d2d(1, h_send, h_recv)
    to_other.start()
    gram[pl.ds(pl.multiple_of(c * width, width), width), :] = total[:, :width]

    for k in range(1, n_s):
        brick_copy(k).wait_recv()
    own_bricks.wait()
    to_other.wait()
    gram[pl.ds(pl.multiple_of((1 - c) * width, width), width), :] = h_recv[...]
    for hop in range(1, n):
        for q in range(PIECES):
            for way in range(2):
                ring_copy(way, hop, q).wait_send()
    for k in range(1, n_s):
        brick_copy(k).wait_send()
    for k in range(1, n_r):
        rs_copy(0, k, (z + k) % n_r).wait_send()


def place_bricks(n_bricks, order, src, dst, buf, in_sem, out_sem):
    tall = src.shape[0] // n_bricks
    group = n_bricks // GROUPS

    def fetch(i):
        return pltpu.make_async_copy(
            src.at[pl.ds(pl.multiple_of(order[0, i] * tall, tall), tall)],
            buf.at[pl.ds(pl.multiple_of(i * tall, tall), tall)],
            in_sem.at[i],
        )

    def put(g):
        block = pl.ds(g * group * tall, group * tall)
        return pltpu.make_async_copy(buf.at[block], dst.at[block], out_sem.at[g])

    def start(i, carry):
        fetch(i).start()
        return carry

    def wait(i, carry):
        fetch(i).wait()
        return carry

    lax.fori_loop(0, n_bricks, start, 0)
    for g in range(GROUPS):
        lax.fori_loop(g * group, (g + 1) * group, wait, 0)
        put(g).start()
    for g in range(GROUPS):
        put(g).wait()


def per_device(n_r, n_s, snapshots, weights, next_bricks, brick_source):
    rows, width = snapshots.shape
    n = n_s // 2
    assert n == n_r and n % 2 == 0
    f32, bf16 = jnp.float32, jnp.bfloat16
    vmem = pl.BlockSpec(memory_space=pltpu.VMEM)
    dma = pltpu.SemaphoreType.DMA
    gram, arrived = pl.pallas_call(
        functools.partial(kernel, n_r, n_s, math.sqrt(rows * n_r)),
        out_shape=(
            jax.ShapeDtypeStruct((n_s * width // n_r, width), f32),
            jax.ShapeDtypeStruct((rows, width), f32),
        ),
        in_specs=[vmem, vmem, vmem],
        out_specs=(vmem, pl.BlockSpec(memory_space=pl.ANY)),
        scratch_shapes=[
            pltpu.VMEM((n - 1, rows, width), f32),
            pltpu.VMEM((rows, width), f32),
            pltpu.VMEM((rows, 2 * width), bf16),
            pltpu.VMEM((rows, 2 * width), bf16),
            pltpu.VMEM((n, width, 2 * width), f32),
            pltpu.VMEM((n_r - 1, width, 2 * width), f32),
            pltpu.VMEM((width, width), f32),
            pltpu.VMEM((width, width), f32),
            dma((2, n - 1, PIECES)),
            dma((2, n - 1, PIECES)),
            dma((n_s - 1,)),
            dma((n_s - 1,)),
            dma((n_r - 1,)),
            dma((n_r - 1,)),
            dma((2,)),
            dma((2,)),
            dma((1,)),
        ],
        compiler_params=pltpu.CompilerParams(
            collective_id=0, has_side_effects=True, vmem_limit_bytes=62 * 1024 * 1024
        ),
    )(snapshots, weights.reshape(-1, 128), next_bricks)
    n_bricks = brick_source.shape[1]
    tiles = pl.pallas_call(
        functools.partial(place_bricks, n_bricks),
        out_shape=jax.ShapeDtypeStruct((rows, width), f32),
        in_specs=[pl.BlockSpec(memory_space=pltpu.SMEM), pl.BlockSpec(memory_space=pl.ANY)],
        out_specs=pl.BlockSpec(memory_space=pl.ANY),
        scratch_shapes=[pltpu.VMEM((rows, width), f32), dma((n_bricks,)), dma((GROUPS,))],
    )(brick_source, arrived)
    return gram, tiles


def solution(mesh):
    placed = (P("rows", "snaps"), P("rows"), P(("rows", "snaps"), None), P("rows", None))
    return jax.shard_map(
        functools.partial(per_device, mesh.shape["rows"], mesh.shape["snaps"]),
        mesh=mesh,
        in_specs=placed,
        out_specs=(P("rows", "snaps"), P("rows", "snaps")),
        check_vma=False,
    )
```

```python
import functools
import math

import jax
import jax.numpy as jnp
from jax import lax
from jax.experimental import pallas as pl
from jax.experimental.pallas import tpu as pltpu
from jax.sharding import PartitionSpec as P

MESH = pl.DeviceIdType.MESH
STEP = 256
PIECES = 2
GROUPS = 8


def split(x):
    hi = x.astype(jnp.bfloat16)
    return hi, (x - hi.astype(jnp.float32)).astype(jnp.bfloat16)


def tdot(a, b):
    return lax.dot_general(a, b, (((0,), (0,)), ((), ())), preferred_element_type=jnp.float32)


def kernel(
    n_r, n_s, scale,
    snap, wts, bricks,
    gram, arrived,
    gbuf, mate, w_hi, w_lo, part, rs_buf, h_send, h_recv,
    ring_send, ring_recv, brick_send, brick_recv, rs_send, rs_recv, d_send, d_recv, own_sem,
):
    n = n_s // 2
    z = lax.axis_index("rows")
    s = lax.axis_index("snaps")
    c = s % 2
    chip = s // 2
    rows, width = snap.shape
    per_brick_dev = bricks.shape[0]

    def ring_of(i):
        u, v = i // 2, i % 2
        return u + v * (n - 1 - 2 * u)

    def chip_at(t):
        v = t // (n // 2)
        return 2 * (t + v * (n - 1 - 2 * t)) + v

    t = ring_of(chip)
    partner = chip * 2 + (1 - c)
    nxt = chip_at((t + 1) % n) * 2 + c
    prv = chip_at((t + n - 1) % n) * 2 + c

    barrier = pltpu.get_barrier_semaphore()
    for k in range(1, n_s):
        pl.semaphore_signal(barrier, inc=1, device_id=(z, (s + k) % n_s), device_id_type=MESH)
    for k in range(1, n_r):
        pl.semaphore_signal(barrier, inc=1, device_id=((z + k) % n_r, s), device_id_type=MESH)
    pl.semaphore_wait(barrier, n_s - 1 + n_r - 1)

    half = rows // 2
    piece = half // PIECES

    def ring_copy(way, hop, q):
        r0 = way * half + q * piece
        there = (n - hop if way == 0 else hop) - 1
        if hop == 1:
            src = snap.at[pl.ds(r0, piece)]
        else:
            here = (n - hop + 1 if way == 0 else hop - 1) - 1
            src = gbuf.at[here, pl.ds(r0, piece)]
        return pltpu.make_async_remote_copy(
            src_ref=src,
            dst_ref=gbuf.at[there, pl.ds(r0, piece)],
            send_sem=ring_send.at[way, hop - 1, q],
            recv_sem=ring_recv.at[way, hop - 1, q],
            device_id=(z, nxt if way == 0 else prv),
            device_id_type=MESH,
        )

    def brick_copy(k):
        to = (s + k) % n_s
        return pltpu.make_async_remote_copy(
            src_ref=bricks.at[:, pl.ds(pl.multiple_of(to * width, width), width)],
            dst_ref=arrived.at[pl.ds(pl.multiple_of(s * per_brick_dev, per_brick_dev), per_brick_dev)],
            send_sem=brick_send.at[k - 1],
            recv_sem=brick_recv.at[k - 1],
            device_id=(z, to),
            device_id_type=MESH,
        )

    def rs_copy(slot, k, home):
        return pltpu.make_async_remote_copy(
            src_ref=part.at[slot],
            dst_ref=rs_buf.at[k - 1],
            send_sem=rs_send.at[k - 1],
            recv_sem=rs_recv.at[k - 1],
            device_id=(home, s),
            device_id_type=MESH,
        )

    def d2d(i, src, dst):
        return pltpu.make_async_remote_copy(
            src_ref=src, dst_ref=dst, send_sem=d_send.at[i], recv_sem=d_recv.at[i],
            device_id=(z, partner), device_id_type=MESH,
        )

    for q in range(PIECES):
        for way in range(2):
            ring_copy(way, 1, q).start()
    own_bricks = pltpu.make_async_copy(
        bricks.at[:, pl.ds(pl.multiple_of(s * width, width), width)],
        arrived.at[pl.ds(pl.multiple_of(s * per_brick_dev, per_brick_dev), per_brick_dev)],
        own_sem.at[0],
    )
    own_bricks.start()
    to_mate = d2d(0, snap, mate)
    to_mate.start()

    def weigh(src, col):
        def body(i, carry):
            r0 = pl.multiple_of(i * 128, 128)
            w = jnp.broadcast_to(wts[pl.ds(i, 1), :], (128, 128)).T
            for l in range(width // 128):
                hi, lo = split(src[pl.ds(r0, 128), l * 128:(l + 1) * 128] * w)
                w_hi[pl.ds(r0, 128), col + l * 128:col + (l + 1) * 128] = hi
                w_lo[pl.ds(r0, 128), col + l * 128:col + (l + 1) * 128] = lo
            return carry
        lax.fori_loop(0, rows // 128, body, 0)

    def gather_product(slot, load, r0, count):
        def body(i, carry):
            r = pl.multiple_of(r0 + i * STEP, STEP)
            hi, lo = split(load(r))
            bh = w_hi[pl.ds(r, STEP), :]
            bl = w_lo[pl.ds(r, STEP), :]
            part[slot] += tdot(hi, bh) + (tdot(hi, bl) + tdot(lo, bh))
            return carry
        lax.fori_loop(0, count // STEP, body, 0)

    def send_home(slot):
        home = chip_at((t + slot) % n)
        k = (home + n_r - z) % n_r

        @pl.when(k > 0)
        def _():
            rs_copy(slot, k, home).start()

    weigh(snap, 0)
    part[...] = jnp.zeros_like(part)
    to_mate.wait()
    weigh(mate, width)
    gather_product(0, lambda r: snap[pl.ds(r, STEP), :], 0, rows)
    send_home(0)

    done = [0] * n
    for hop in range(1, n):
        for q in range(PIECES):
            for way in range(2):
                ring_copy(way, hop, q).wait_recv()
                if hop < n - 1:
                    ring_copy(way, hop + 1, q).start()
            if q == PIECES - 1 and hop == n - 2:
                for k in range(1, n_s):
                    brick_copy(k).start()
            for way in range(2):
                slot = n - hop if way == 0 else hop
                gather_product(
                    slot,
                    lambda r, slot=slot: gbuf[slot - 1, pl.ds(r, STEP), :],
                    way * half + q * piece,
                    piece,
                )
        for way in range(2):
            slot = n - hop if way == 0 else hop
            done[slot] += 1
            if done[slot] == 2:
                send_home(slot)

    for k in range(1, n_r):
        rs_copy(0, k, (z + k) % n_r).wait_recv()
    own = (ring_of(z) + n - t) % n
    total = part[own]
    for k in range(1, n_r):
        total += rs_buf[k - 1]
    total = total / scale
    h_send[...] = total[:, width:]
    to_other = d2d(1, h_send, h_recv)
    to_other.start()
    gram[pl.ds(pl.multiple_of(c * width, width), width), :] = total[:, :width]

    for k in range(1, n_s):
        brick_copy(k).wait_recv()
    own_bricks.wait()
    to_other.wait()
    gram[pl.ds(pl.multiple_of((1 - c) * width, width), width), :] = h_recv[...]
    for hop in range(1, n):
        for q in range(PIECES):
            for way in range(2):
                ring_copy(way, hop, q).wait_send()
    for k in range(1, n_s):
        brick_copy(k).wait_send()
    for k in range(1, n_r):
        rs_copy(0, k, (z + k) % n_r).wait_send()


def folded_kernel(
    n_r, n_s, scale,
    snap, wts, bricks,
    gram, arrived,
    gbuf, mate, w_hi, w_lo, part, rs_buf, quad, xbuf, fin, fbuf,
    ring_send, ring_recv, brick_send, brick_recv, rs_send, rs_recv,
    x_send, x_recv, f_send, f_recv, d_send, d_recv, own_sem,
):
    n = n_s // 2
    z = lax.axis_index("rows")
    s = lax.axis_index("snaps")
    c = s % 2
    chip = s // 2
    rows, width = snap.shape
    per_brick_dev = bricks.shape[0]

    def ring_of(i):
        u, v = i // 2, i % 2
        return u + v * (n - 1 - 2 * u)

    def chip_at(t):
        v = t // (n // 2)
        return 2 * (t + v * (n - 1 - 2 * t)) + v

    t = ring_of(chip)
    partner = chip * 2 + (1 - c)
    nxt = chip_at((t + 1) % n) * 2 + c
    prv = chip_at((t + n - 1) % n) * 2 + c

    barrier = pltpu.get_barrier_semaphore()
    for k in range(1, n_s):
        pl.semaphore_signal(barrier, inc=1, device_id=(z, (s + k) % n_s), device_id_type=MESH)
    for k in range(1, n_r):
        for who in (s, partner):
            pl.semaphore_signal(barrier, inc=1, device_id=((z + k) % n_r, who), device_id_type=MESH)
    pl.semaphore_wait(barrier, n_s - 1 + 2 * (n_r - 1))

    half = rows // 2
    piece = half // 2

    def start_of(way, owner, other):
        q = owner // 2
        q = q + other * (1 - 2 * q)
        return pl.multiple_of(way * half + q * piece, piece)

    def ring_copy(way, stage):
        if stage < 2:
            r0 = start_of(way, t, stage)
            src = snap.at[pl.ds(r0, piece)]
            there = n - 1 if way == 0 else 1
        else:
            owner = (t + n - 1) % n if way == 0 else (t + 1) % n
            r0 = start_of(way, owner, 0)
            src = gbuf.at[n - 2 if way == 0 else 0, pl.ds(r0, piece)]
            there = 2
        return pltpu.make_async_remote_copy(
            src_ref=src,
            dst_ref=gbuf.at[there - 1, pl.ds(r0, piece)],
            send_sem=ring_send.at[way, stage],
            recv_sem=ring_recv.at[way, stage],
            device_id=(z, nxt if way == 0 else prv),
            device_id_type=MESH,
        )

    def brick_copy(k):
        to = (s + k) % n_s
        return pltpu.make_async_remote_copy(
            src_ref=bricks.at[:, pl.ds(pl.multiple_of(to * width, width), width)],
            dst_ref=arrived.at[pl.ds(pl.multiple_of(s * per_brick_dev, per_brick_dev), per_brick_dev)],
            send_sem=brick_send.at[k - 1],
            recv_sem=brick_recv.at[k - 1],
            device_id=(z, to),
            device_id_type=MESH,
        )

    def level_of(other, row_core, col_core):
        low = jnp.where(chip <= other, 1, 0)
        return low * (2 * row_core + col_core) + (1 - low) * (2 * col_core + row_core)

    def chunk(d):
        return chip_at((t + d) % n)

    def col_core_here(d):
        low = jnp.where(chip <= chunk(d), 1, 0)
        return low * (z % 2) + (1 - low) * (z // 2)

    def holds(d):
        low = jnp.where(chip <= chunk(d), 1, 0)
        return low * (z // 2) + (1 - low) * (z % 2) == c

    def rs_copy(d, side, k, home):
        return pltpu.make_async_remote_copy(
            src_ref=part.at[d, :, pl.ds(side * width, width)],
            dst_ref=rs_buf.at[d, k - 1],
            send_sem=rs_send.at[d, side],
            recv_sem=rs_recv.at[d, k - 1],
            device_id=(home, s),
            device_id_type=MESH,
        )

    def x_copy(d):
        return pltpu.make_async_remote_copy(
            src_ref=quad.at[d],
            dst_ref=xbuf.at[n - d - 1],
            send_sem=x_send.at[d - 1],
            recv_sem=x_recv.at[n - d - 1],
            device_id=(z, chunk(d) * 2 + col_core_here(d)),
            device_id_type=MESH,
        )

    def x_arrival(d):
        return pltpu.make_async_remote_copy(
            src_ref=quad.at[d],
            dst_ref=xbuf.at[d - 1],
            send_sem=x_send.at[d - 1],
            recv_sem=x_recv.at[d - 1],
            device_id=(z, chunk(d) * 2 + col_core_here(d)),
            device_id_type=MESH,
        )

    def f_copy(d):
        return pltpu.make_async_remote_copy(
            src_ref=fin.at[d],
            dst_ref=fbuf.at[c],
            send_sem=f_send.at[d],
            recv_sem=f_recv.at[c],
            device_id=(chunk(d), chip * 2 + col_core_here(d)),
            device_id_type=MESH,
        )

    def f_arrival(a):
        return pltpu.make_async_remote_copy(
            src_ref=fin.at[0],
            dst_ref=fbuf.at[a],
            send_sem=f_send.at[0],
            recv_sem=f_recv.at[a],
            device_id=((z + 1) % n_r, s),
            device_id_type=MESH,
        )

    for stage in range(2):
        for way in range(2):
            ring_copy(way, stage).start()
    own_bricks = pltpu.make_async_copy(
        bricks.at[:, pl.ds(pl.multiple_of(s * width, width), width)],
        arrived.at[pl.ds(pl.multiple_of(s * per_brick_dev, per_brick_dev), per_brick_dev)],
        own_sem.at[0],
    )
    own_bricks.start()
    to_mate = pltpu.make_async_remote_copy(
        src_ref=snap, dst_ref=mate, send_sem=d_send.at[0], recv_sem=d_recv.at[0],
        device_id=(z, partner), device_id_type=MESH,
    )
    to_mate.start()

    def weigh(src, col):
        def body(i, carry):
            r0 = pl.multiple_of(i * 128, 128)
            w = jnp.broadcast_to(wts[pl.ds(i, 1), :], (128, 128)).T
            for l in range(width // 128):
                hi, lo = split(src[pl.ds(r0, 128), l * 128:(l + 1) * 128] * w)
                w_hi[pl.ds(r0, 128), col + l * 128:col + (l + 1) * 128] = hi
                w_lo[pl.ds(r0, 128), col + l * 128:col + (l + 1) * 128] = lo
            return carry
        lax.fori_loop(0, rows // 128, body, 0)

    def gather_product(slot, load, r0, count):
        def body(i, carry):
            r = pl.multiple_of(r0 + i * STEP, STEP)
            hi, lo = split(load(r))
            bh = w_hi[pl.ds(r, STEP), :]
            bl = w_lo[pl.ds(r, STEP), :]
            part[slot] += tdot(hi, bh) + (tdot(hi, bl) + tdot(lo, bh))
            return carry
        lax.fori_loop(0, count // STEP, body, 0)

    def take(slot, r0):
        gather_product(slot, lambda r: gbuf[slot - 1, pl.ds(r, STEP), :], r0, piece)

    def sides(d, act):
        for side in range(2):
            home = level_of(chunk(d), c, (c + side) % 2)
            k = (home + n_r - z) % n_r

            @pl.when(k > 0)
            def _():
                act(rs_copy(d, side, k, home))

    weigh(snap, 0)
    part[...] = jnp.zeros_like(part)
    to_mate.wait()
    weigh(mate, width)
    gather_product(0, lambda r: snap[pl.ds(r, STEP), :], 0, rows)
    sides(0, lambda copy: copy.start())

    near = ((0, n - 1, (t + n - 1) % n), (1, 1, (t + 1) % n))
    for way, slot, owner in near:
        ring_copy(way, 0).wait_recv()
        ring_copy(way, 2).start()
    for way, slot, owner in near:
        take(slot, start_of(way, owner, 0))
    for way, slot, owner in near:
        ring_copy(way, 1).wait_recv()
    for k in range(1, n_s):
        brick_copy(k).start()
    for way, slot, owner in near:
        take(slot, start_of(way, owner, 1))
        sides(slot, lambda copy: copy.start())
    for way in range(2):
        ring_copy(way, 2).wait_recv()
        take(2, start_of(way, (t + 2) % n, 0))
    sides(2, lambda copy: copy.start())

    def finish(d):
        col_core = col_core_here(d)
        home = chunk(d)
        here = jnp.where(home == z, 1, 0) * jnp.where(col_core == c, 1, 0)

        @pl.when(here == 0)
        def _():
            f_copy(d).start()

        @pl.when(here == 1)
        def _():
            fbuf[c] = fin[d]

    order = (0, 1, 3, 2)
    for d in order:
        @pl.when(holds(d))
        def _():
            for k in range(1, n_r):
                rs_copy(d, 0, k, (z + k) % n_r).wait_recv()
            side = (col_core_here(d) + c) % 2
            total = part[d, :, pl.ds(pl.multiple_of(side * width, width), width)]
            for k in range(1, n_r):
                total += rs_buf[d, k - 1]
            if d == 0:
                fin[0] = total / scale
                finish(0)
            else:
                quad[d] = total
                x_copy(d).start()
    for d in order[1:]:
        @pl.when(holds(d))
        def _():
            x_arrival(d).wait_recv()
            fin[d] = (quad[d] + xbuf[d - 1].T) / scale
            finish(d)

    for k in range(1, n_s):
        brick_copy(k).wait_recv()
    own_bricks.wait()
    for a in range(2):
        level = level_of(z, a, c)
        same = jnp.where(level == z, 1, 0) * jnp.where(c == a, 1, 0)

        @pl.when(same == 0)
        def _():
            f_arrival(a).wait_recv()

        gram[a * width:(a + 1) * width, :] = fbuf[a]

    for way in range(2):
        for stage in range(3):
            ring_copy(way, stage).wait_send()
    for k in range(1, n_s):
        brick_copy(k).wait_send()
    for d in range(n):
        sides(d, lambda copy: copy.wait_send())

        @pl.when(holds(d))
        def _():
            if d > 0:
                x_copy(d).wait_send()
            here = jnp.where(chunk(d) == z, 1, 0) * jnp.where(col_core_here(d) == c, 1, 0)

            @pl.when(here == 0)
            def _():
                f_copy(d).wait_send()


def place_bricks(n_bricks, order, src, dst, buf, in_sem, out_sem):
    tall = src.shape[0] // n_bricks
    group = n_bricks // GROUPS

    def fetch(i):
        return pltpu.make_async_copy(
            src.at[pl.ds(pl.multiple_of(order[0, i] * tall, tall), tall)],
            buf.at[pl.ds(pl.multiple_of(i * tall, tall), tall)],
            in_sem.at[i],
        )

    def put(g):
        block = pl.ds(g * group * tall, group * tall)
        return pltpu.make_async_copy(buf.at[block], dst.at[block], out_sem.at[g])

    def start(i, carry):
        fetch(i).start()
        return carry

    def wait(i, carry):
        fetch(i).wait()
        return carry

    lax.fori_loop(0, n_bricks, start, 0)
    for g in range(GROUPS):
        lax.fori_loop(g * group, (g + 1) * group, wait, 0)
        put(g).start()
    for g in range(GROUPS):
        put(g).wait()


def per_device(n_r, n_s, snapshots, weights, next_bricks, brick_source):
    rows, width = snapshots.shape
    n = n_s // 2
    assert n == n_r and n % 2 == 0
    f32, bf16 = jnp.float32, jnp.bfloat16
    vmem = pl.BlockSpec(memory_space=pltpu.VMEM)
    dma = pltpu.SemaphoreType.DMA
    wide = 2 * width
    scratch = [
        pltpu.VMEM((n - 1, rows, width), f32),
        pltpu.VMEM((rows, width), f32),
        pltpu.VMEM((rows, wide), bf16),
        pltpu.VMEM((rows, wide), bf16),
        pltpu.VMEM((n, width, wide), f32),
    ]
    folded = n == 4
    if folded:
        scratch += [
            pltpu.VMEM((n, n_r - 1, width, width), f32),
            pltpu.VMEM((n, width, width), f32),
            pltpu.VMEM((n - 1, width, width), f32),
            pltpu.VMEM((n, width, width), f32),
            pltpu.VMEM((2, width, width), f32),
            dma((2, 3)),
            dma((2, 3)),
            dma((n_s - 1,)),
            dma((n_s - 1,)),
            dma((n, 2)),
            dma((n, n_r - 1)),
            dma((n - 1,)),
            dma((n - 1,)),
            dma((n,)),
            dma((2,)),
            dma((1,)),
            dma((1,)),
            dma((1,)),
        ]
    else:
        scratch += [
            pltpu.VMEM((n_r - 1, width, wide), f32),
            pltpu.VMEM((width, width), f32),
            pltpu.VMEM((width, width), f32),
            dma((2, n - 1, PIECES)),
            dma((2, n - 1, PIECES)),
            dma((n_s - 1,)),
            dma((n_s - 1,)),
            dma((n_r - 1,)),
            dma((n_r - 1,)),
            dma((2,)),
            dma((2,)),
            dma((1,)),
        ]
    gram, arrived = pl.pallas_call(
        functools.partial(folded_kernel if folded else kernel, n_r, n_s, math.sqrt(rows * n_r)),
        out_shape=(
            jax.ShapeDtypeStruct((n_s * width // n_r, width), f32),
            jax.ShapeDtypeStruct((rows, width), f32),
        ),
        in_specs=[vmem, vmem, vmem],
        out_specs=(vmem, pl.BlockSpec(memory_space=pl.ANY)),
        scratch_shapes=scratch,
        compiler_params=pltpu.CompilerParams(
            collective_id=0, has_side_effects=True, vmem_limit_bytes=62 * 1024 * 1024
        ),
    )(snapshots, weights.reshape(-1, 128), next_bricks)
    n_bricks = brick_source.shape[1]
    tiles = pl.pallas_call(
        functools.partial(place_bricks, n_bricks),
        out_shape=jax.ShapeDtypeStruct((rows, width), f32),
        in_specs=[pl.BlockSpec(memory_space=pltpu.SMEM), pl.BlockSpec(memory_space=pl.ANY)],
        out_specs=pl.BlockSpec(memory_space=pl.ANY),
        scratch_shapes=[pltpu.VMEM((rows, width), f32), dma((n_bricks,)), dma((GROUPS,))],
    )(brick_source, arrived)
    return gram, tiles


def solution(mesh):
    placed = (P("rows", "snaps"), P("rows"), P(("rows", "snaps"), None), P("rows", None))
    return jax.shard_map(
        functools.partial(per_device, mesh.shape["rows"], mesh.shape["snaps"]),
        mesh=mesh,
        in_specs=placed,
        out_specs=(P("rows", "snaps"), P("rows", "snaps")),
        check_vma=False,
    )
```

```python
import functools
import math

import jax
import jax.numpy as jnp
from jax import lax
from jax.experimental import pallas as pl
from jax.experimental.pallas import tpu as pltpu
from jax.sharding import PartitionSpec as P

MESH = pl.DeviceIdType.MESH
STEP = 256
PIECES = 2
GROUPS = 8


def split(x):
    hi = x.astype(jnp.bfloat16)
    return hi, (x - hi.astype(jnp.float32)).astype(jnp.bfloat16)


def tdot(a, b):
    return lax.dot_general(a, b, (((0,), (0,)), ((), ())), preferred_element_type=jnp.float32)


def kernel(
    n_r, n_s, scale,
    snap, wts, bricks,
    gram, arrived,
    gbuf, mate, w_hi, w_lo, part, rs_buf, h_send, h_recv,
    ring_send, ring_recv, brick_send, brick_recv, rs_send, rs_recv, d_send, d_recv, own_sem,
):
    n = n_s // 2
    z = lax.axis_index("rows")
    s = lax.axis_index("snaps")
    c = s % 2
    chip = s // 2
    rows, width = snap.shape
    per_brick_dev = bricks.shape[0]

    def ring_of(i):
        u, v = i // 2, i % 2
        return u + v * (n - 1 - 2 * u)

    def chip_at(t):
        v = t // (n // 2)
        return 2 * (t + v * (n - 1 - 2 * t)) + v

    t = ring_of(chip)
    partner = chip * 2 + (1 - c)
    nxt = chip_at((t + 1) % n) * 2 + c
    prv = chip_at((t + n - 1) % n) * 2 + c

    barrier = pltpu.get_barrier_semaphore()
    for k in range(1, n_s):
        pl.semaphore_signal(barrier, inc=1, device_id=(z, (s + k) % n_s), device_id_type=MESH)
    for k in range(1, n_r):
        pl.semaphore_signal(barrier, inc=1, device_id=((z + k) % n_r, s), device_id_type=MESH)
    pl.semaphore_wait(barrier, n_s - 1 + n_r - 1)

    half = rows // 2
    piece = half // PIECES

    def ring_copy(way, hop, q):
        r0 = way * half + q * piece
        there = (n - hop if way == 0 else hop) - 1
        if hop == 1:
            src = snap.at[pl.ds(r0, piece)]
        else:
            here = (n - hop + 1 if way == 0 else hop - 1) - 1
            src = gbuf.at[here, pl.ds(r0, piece)]
        return pltpu.make_async_remote_copy(
            src_ref=src,
            dst_ref=gbuf.at[there, pl.ds(r0, piece)],
            send_sem=ring_send.at[way, hop - 1, q],
            recv_sem=ring_recv.at[way, hop - 1, q],
            device_id=(z, nxt if way == 0 else prv),
            device_id_type=MESH,
        )

    def brick_copy(k):
        to = (s + k) % n_s
        return pltpu.make_async_remote_copy(
            src_ref=bricks.at[:, pl.ds(pl.multiple_of(to * width, width), width)],
            dst_ref=arrived.at[pl.ds(pl.multiple_of(s * per_brick_dev, per_brick_dev), per_brick_dev)],
            send_sem=brick_send.at[k - 1],
            recv_sem=brick_recv.at[k - 1],
            device_id=(z, to),
            device_id_type=MESH,
        )

    def rs_copy(slot, k, home):
        return pltpu.make_async_remote_copy(
            src_ref=part.at[slot],
            dst_ref=rs_buf.at[k - 1],
            send_sem=rs_send.at[k - 1],
            recv_sem=rs_recv.at[k - 1],
            device_id=(home, s),
            device_id_type=MESH,
        )

    def d2d(i, src, dst):
        return pltpu.make_async_remote_copy(
            src_ref=src, dst_ref=dst, send_sem=d_send.at[i], recv_sem=d_recv.at[i],
            device_id=(z, partner), device_id_type=MESH,
        )

    for q in range(PIECES):
        for way in range(2):
            ring_copy(way, 1, q).start()
    own_bricks = pltpu.make_async_copy(
        bricks.at[:, pl.ds(pl.multiple_of(s * width, width), width)],
        arrived.at[pl.ds(pl.multiple_of(s * per_brick_dev, per_brick_dev), per_brick_dev)],
        own_sem.at[0],
    )
    own_bricks.start()
    to_mate = d2d(0, snap, mate)
    to_mate.start()

    def weigh(src, col):
        def body(i, carry):
            r0 = pl.multiple_of(i * 128, 128)
            w = jnp.broadcast_to(wts[pl.ds(i, 1), :], (128, 128)).T
            for l in range(width // 128):
                hi, lo = split(src[pl.ds(r0, 128), l * 128:(l + 1) * 128] * w)
                w_hi[pl.ds(r0, 128), col + l * 128:col + (l + 1) * 128] = hi
                w_lo[pl.ds(r0, 128), col + l * 128:col + (l + 1) * 128] = lo
            return carry
        lax.fori_loop(0, rows // 128, body, 0)

    def gather_product(slot, load, r0, count):
        def body(i, carry):
            r = pl.multiple_of(r0 + i * STEP, STEP)
            hi, lo = split(load(r))
            bh = w_hi[pl.ds(r, STEP), :]
            bl = w_lo[pl.ds(r, STEP), :]
            part[slot] += tdot(hi, bh) + (tdot(hi, bl) + tdot(lo, bh))
            return carry
        lax.fori_loop(0, count // STEP, body, 0)

    def send_home(slot):
        home = chip_at((t + slot) % n)
        k = (home + n_r - z) % n_r

        @pl.when(k > 0)
        def _():
            rs_copy(slot, k, home).start()

    weigh(snap, 0)
    part[...] = jnp.zeros_like(part)
    to_mate.wait()
    weigh(mate, width)
    gather_product(0, lambda r: snap[pl.ds(r, STEP), :], 0, rows)
    send_home(0)

    done = [0] * n
    for hop in range(1, n):
        for q in range(PIECES):
            for way in range(2):
                ring_copy(way, hop, q).wait_recv()
                if hop < n - 1:
                    ring_copy(way, hop + 1, q).start()
            if q == PIECES - 1 and hop == n - 2:
                for k in range(1, n_s):
                    brick_copy(k).start()
            for way in range(2):
                slot = n - hop if way == 0 else hop
                gather_product(
                    slot,
                    lambda r, slot=slot: gbuf[slot - 1, pl.ds(r, STEP), :],
                    way * half + q * piece,
                    piece,
                )
        for way in range(2):
            slot = n - hop if way == 0 else hop
            done[slot] += 1
            if done[slot] == 2:
                send_home(slot)

    for k in range(1, n_r):
        rs_copy(0, k, (z + k) % n_r).wait_recv()
    own = (ring_of(z) + n - t) % n
    total = part[own]
    for k in range(1, n_r):
        total += rs_buf[k - 1]
    total = total / scale
    h_send[...] = total[:, width:]
    to_other = d2d(1, h_send, h_recv)
    to_other.start()
    gram[pl.ds(pl.multiple_of(c * width, width), width), :] = total[:, :width]

    for k in range(1, n_s):
        brick_copy(k).wait_recv()
    own_bricks.wait()
    to_other.wait()
    gram[pl.ds(pl.multiple_of((1 - c) * width, width), width), :] = h_recv[...]
    for hop in range(1, n):
        for q in range(PIECES):
            for way in range(2):
                ring_copy(way, hop, q).wait_send()
    for k in range(1, n_s):
        brick_copy(k).wait_send()
    for k in range(1, n_r):
        rs_copy(0, k, (z + k) % n_r).wait_send()


def folded_kernel(
    n_r, n_s, scale,
    snap_in, wts, bricks,
    gram, arrived,
    snap, bounce, gbuf, mate, w_hi, w_lo, part, rs_buf, quad, xbuf, fin, fbuf,
    ring_send, ring_recv, brick_send, brick_recv, rs_send, rs_recv,
    x_send, x_recv, f_send, f_recv, d_send, d_recv, own_sem, in_sem,
):
    n = n_s // 2
    z = lax.axis_index("rows")
    s = lax.axis_index("snaps")
    c = s % 2
    chip = s // 2
    rows, width = snap_in.shape
    per_brick_dev = bricks.shape[0]

    def ring_of(i):
        u, v = i // 2, i % 2
        return u + v * (n - 1 - 2 * u)

    def chip_at(t):
        v = t // (n // 2)
        return 2 * (t + v * (n - 1 - 2 * t)) + v

    t = ring_of(chip)
    partner = chip * 2 + (1 - c)
    nxt = chip_at((t + 1) % n) * 2 + c
    prv = chip_at((t + n - 1) % n) * 2 + c

    load_snap = pltpu.make_async_copy(snap_in, snap, in_sem.at[0])
    load_snap.start()
    own_bricks_in = pltpu.make_async_copy(
        bricks.at[:, pl.ds(pl.multiple_of(s * width, width), width)], bounce, in_sem.at[1]
    )
    own_bricks_in.start()
    barrier = pltpu.get_barrier_semaphore()
    for k in range(1, n_s):
        pl.semaphore_signal(barrier, inc=1, device_id=(z, (s + k) % n_s), device_id_type=MESH)
    for k in range(1, n_r):
        for who in (s, partner):
            pl.semaphore_signal(barrier, inc=1, device_id=((z + k) % n_r, who), device_id_type=MESH)
    load_snap.wait()
    pl.semaphore_wait(barrier, n_s - 1 + 2 * (n_r - 1))

    half = rows // 2
    piece = half // 2

    def start_of(way, owner, other):
        q = owner // 2
        q = q + other * (1 - 2 * q)
        return pl.multiple_of(way * half + q * piece, piece)

    def slot_of(way):
        return n - 1 - way * (n - 2)

    def owner_of(way):
        return (t + n - 1 + 2 * way) % n

    def ring_copy(way, stage):
        if stage < 2:
            r0 = start_of(way, t, stage)
            src = snap.at[pl.ds(r0, piece)]
            there = n - 1 - way * (n - 2)
        else:
            owner = owner_of(way)
            r0 = start_of(way, owner, 0)
            src = gbuf.at[slot_of(way) - 1, pl.ds(r0, piece)]
            there = 2
        return pltpu.make_async_remote_copy(
            src_ref=src,
            dst_ref=gbuf.at[there - 1, pl.ds(r0, piece)],
            send_sem=ring_send.at[way, stage],
            recv_sem=ring_recv.at[way, stage],
            device_id=(z, nxt + way * (prv - nxt)),
            device_id_type=MESH,
        )

    def brick_copy(k):
        to = (s + k) % n_s
        return pltpu.make_async_remote_copy(
            src_ref=bricks.at[:, pl.ds(pl.multiple_of(to * width, width), width)],
            dst_ref=arrived.at[pl.ds(pl.multiple_of(s * per_brick_dev, per_brick_dev), per_brick_dev)],
            send_sem=brick_send.at[k - 1],
            recv_sem=brick_recv.at[k - 1],
            device_id=(z, to),
            device_id_type=MESH,
        )

    def level_of(other, row_core, col_core):
        low = jnp.where(chip <= other, 1, 0)
        return low * (2 * row_core + col_core) + (1 - low) * (2 * col_core + row_core)

    def chunk(d):
        return chip_at((t + d) % n)

    def col_core_here(d):
        low = jnp.where(chip <= chunk(d), 1, 0)
        return low * (z % 2) + (1 - low) * (z // 2)

    def holds(d):
        low = jnp.where(chip <= chunk(d), 1, 0)
        return low * (z // 2) + (1 - low) * (z % 2) == c

    def rs_copy(d, side, k, home):
        return pltpu.make_async_remote_copy(
            src_ref=part.at[d, :, pl.ds(side * width, width)],
            dst_ref=rs_buf.at[d, k - 1],
            send_sem=rs_send.at[d, side],
            recv_sem=rs_recv.at[d, k - 1],
            device_id=(home, s),
            device_id_type=MESH,
        )

    def x_copy(d):
        return pltpu.make_async_remote_copy(
            src_ref=quad.at[d],
            dst_ref=xbuf.at[n - d - 1],
            send_sem=x_send.at[d - 1],
            recv_sem=x_recv.at[n - d - 1],
            device_id=(z, chunk(d) * 2 + col_core_here(d)),
            device_id_type=MESH,
        )

    def x_arrival(d):
        return pltpu.make_async_remote_copy(
            src_ref=quad.at[d],
            dst_ref=xbuf.at[d - 1],
            send_sem=x_send.at[d - 1],
            recv_sem=x_recv.at[d - 1],
            device_id=(z, chunk(d) * 2 + col_core_here(d)),
            device_id_type=MESH,
        )

    def f_copy(d):
        return pltpu.make_async_remote_copy(
            src_ref=fin.at[d],
            dst_ref=fbuf.at[c],
            send_sem=f_send.at[d],
            recv_sem=f_recv.at[c],
            device_id=(chunk(d), chip * 2 + col_core_here(d)),
            device_id_type=MESH,
        )

    def f_arrival(a):
        return pltpu.make_async_remote_copy(
            src_ref=fin.at[0],
            dst_ref=fbuf.at[a],
            send_sem=f_send.at[0],
            recv_sem=f_recv.at[a],
            device_id=((z + 1) % n_r, s),
            device_id_type=MESH,
        )

    first, second = c, 1 - c
    for stage in range(2):
        ring_copy(first, stage).start()
    own_bricks_in.wait()
    own_bricks = pltpu.make_async_copy(
        bounce,
        arrived.at[pl.ds(pl.multiple_of(s * per_brick_dev, per_brick_dev), per_brick_dev)],
        own_sem.at[0],
    )
    own_bricks.start()
    to_mate = pltpu.make_async_remote_copy(
        src_ref=snap, dst_ref=mate, send_sem=d_send.at[0], recv_sem=d_recv.at[0],
        device_id=(z, partner), device_id_type=MESH,
    )
    to_mate.start()

    def weigh(src, col):
        def body(i, carry):
            r0 = pl.multiple_of(i * 128, 128)
            w = jnp.broadcast_to(wts[pl.ds(i, 1), :], (128, 128)).T
            for l in range(width // 128):
                hi, lo = split(src[pl.ds(r0, 128), l * 128:(l + 1) * 128] * w)
                w_hi[pl.ds(r0, 128), col + l * 128:col + (l + 1) * 128] = hi
                w_lo[pl.ds(r0, 128), col + l * 128:col + (l + 1) * 128] = lo
            return carry
        lax.fori_loop(0, rows // 128, body, 0)

    def gather_product(slot, load, r0, count):
        def body(i, carry):
            r = pl.multiple_of(r0 + i * STEP, STEP)
            hi, lo = split(load(r))
            bh = w_hi[pl.ds(r, STEP), :]
            bl = w_lo[pl.ds(r, STEP), :]
            part[slot] += tdot(hi, bh) + (tdot(hi, bl) + tdot(lo, bh))
            return carry
        lax.fori_loop(0, count // STEP, body, 0)

    def take(slot, r0):
        gather_product(slot, lambda r: gbuf[slot - 1, pl.ds(r, STEP), :], r0, piece)

    def sides(d, act):
        for side in range(2):
            home = level_of(chunk(d), c, (c + side) % 2)
            k = (home + n_r - z) % n_r

            @pl.when(k > 0)
            def _():
                act(rs_copy(d, side, k, home))

    weigh(snap, 0)
    part[...] = jnp.zeros_like(part)
    to_mate.wait()
    weigh(mate, width)
    gather_product(0, lambda r: snap[pl.ds(r, STEP), :], 0, rows)
    sides(0, lambda copy: copy.start())

    def finish(d):
        col_core = col_core_here(d)
        home = chunk(d)
        here = jnp.where(home == z, 1, 0) * jnp.where(col_core == c, 1, 0)

        @pl.when(here == 0)
        def _():
            f_copy(d).start()

        @pl.when(here == 1)
        def _():
            fbuf[c] = fin[d]

    def reduce_quadrant(d):
        @pl.when(holds(d))
        def _():
            for k in range(1, n_r):
                rs_copy(d, 0, k, (z + k) % n_r).wait_recv()
            side = (col_core_here(d) + c) % 2
            total = part[d, :, pl.ds(pl.multiple_of(side * width, width), width)]
            for k in range(1, n_r):
                total += rs_buf[d, k - 1]
            if d == 0:
                fin[0] = total / scale
                finish(0)
            else:
                quad[d] = total
                x_copy(d).start()
    def near(way):
        for stage in range(2):
            ring_copy(way, stage).wait_recv()
        slot = slot_of(way)
        for stage in range(2):
            take(slot, start_of(way, owner_of(way), stage))
        sides(slot, lambda copy: copy.start())

    for stage in range(2):
        ring_copy(first, stage).wait_send()
        ring_copy(second, stage).start()
    near(first)
    reduce_quadrant(0)
    for stage in range(2):
        ring_copy(second, stage).wait_send()
        if stage == 0:
            ring_copy(first, 2).start()
    ring_copy(second, 0).wait_recv()
    ring_copy(second, 2).start()
    for k in range(1, n_s):
        brick_copy(k).start()
    ring_copy(second, 1).wait_recv()
    for stage in range(2):
        take(slot_of(second), start_of(second, owner_of(second), stage))
    sides(slot_of(second), lambda copy: copy.start())
    for way in range(2):
        ring_copy(way, 2).wait_recv()
        take(2, start_of(way, (t + 2) % n, 0))
    sides(2, lambda copy: copy.start())

    order = (1, 3, 2)
    for d in order:
        reduce_quadrant(d)
    for d in order:
        @pl.when(holds(d))
        def _():
            x_arrival(d).wait_recv()
            fin[d] = (quad[d] + xbuf[d - 1].T) / scale
            finish(d)

    for k in range(1, n_s):
        brick_copy(k).wait_recv()
    own_bricks.wait()
    for a in range(2):
        level = level_of(z, a, c)
        same = jnp.where(level == z, 1, 0) * jnp.where(c == a, 1, 0)

        @pl.when(same == 0)
        def _():
            f_arrival(a).wait_recv()

        gram[a * width:(a + 1) * width, :] = fbuf[a]

    for way in range(2):
        ring_copy(way, 2).wait_send()
    for k in range(1, n_s):
        brick_copy(k).wait_send()
    for d in range(n):
        sides(d, lambda copy: copy.wait_send())

        @pl.when(holds(d))
        def _():
            if d > 0:
                x_copy(d).wait_send()
            here = jnp.where(chunk(d) == z, 1, 0) * jnp.where(col_core_here(d) == c, 1, 0)

            @pl.when(here == 0)
            def _():
                f_copy(d).wait_send()


def place_bricks(n_bricks, order, src, gram, dst, gram_out, buf, gram_buf, in_sem, out_sem, g_sem):
    gram_in = pltpu.make_async_copy(gram, gram_buf, g_sem.at[0])
    gram_in.start()
    tall = src.shape[0] // n_bricks
    group = n_bricks // GROUPS

    def fetch(i):
        return pltpu.make_async_copy(
            src.at[pl.ds(pl.multiple_of(order[0, i] * tall, tall), tall)],
            buf.at[pl.ds(pl.multiple_of(i * tall, tall), tall)],
            in_sem.at[i],
        )

    def put(g):
        block = pl.ds(g * group * tall, group * tall)
        return pltpu.make_async_copy(buf.at[block], dst.at[block], out_sem.at[g])

    def start(i, carry):
        fetch(i).start()
        return carry

    def wait(i, carry):
        fetch(i).wait()
        return carry

    lax.fori_loop(0, n_bricks, start, 0)
    for g in range(GROUPS):
        lax.fori_loop(g * group, (g + 1) * group, wait, 0)
        put(g).start()
    gram_in.wait()
    gram_put = pltpu.make_async_copy(gram_buf, gram_out, g_sem.at[1])
    gram_put.start()
    for g in range(GROUPS):
        put(g).wait()
    gram_put.wait()


def per_device(n_r, n_s, snapshots, weights, next_bricks, brick_source):
    rows, width = snapshots.shape
    n = n_s // 2
    assert n == n_r and n % 2 == 0
    f32, bf16 = jnp.float32, jnp.bfloat16
    vmem = pl.BlockSpec(memory_space=pltpu.VMEM)
    dma = pltpu.SemaphoreType.DMA
    wide = 2 * width
    hbm = pl.BlockSpec(memory_space=pl.ANY)
    scratch = [
        pltpu.VMEM((n - 1, rows, width), f32),
        pltpu.VMEM((rows, width), f32),
        pltpu.VMEM((rows, wide), bf16),
        pltpu.VMEM((rows, wide), bf16),
        pltpu.VMEM((n, width, wide), f32),
    ]
    folded = n == 4
    if folded:
        scratch = [pltpu.VMEM((rows, width), f32), pltpu.VMEM((rows // n_s, width), f32)] + scratch + [
            pltpu.VMEM((n, n_r - 1, width, width), f32),
            pltpu.VMEM((n, width, width), f32),
            pltpu.VMEM((n - 1, width, width), f32),
            pltpu.VMEM((n, width, width), f32),
            pltpu.VMEM((2, width, width), f32),
            dma((2, 3)),
            dma((2, 3)),
            dma((n_s - 1,)),
            dma((n_s - 1,)),
            dma((n, 2)),
            dma((n, n_r - 1)),
            dma((n - 1,)),
            dma((n - 1,)),
            dma((n,)),
            dma((2,)),
            dma((1,)),
            dma((1,)),
            dma((1,)),
            dma((2,)),
        ]
    else:
        scratch += [
            pltpu.VMEM((n_r - 1, width, wide), f32),
            pltpu.VMEM((width, width), f32),
            pltpu.VMEM((width, width), f32),
            dma((2, n - 1, PIECES)),
            dma((2, n - 1, PIECES)),
            dma((n_s - 1,)),
            dma((n_s - 1,)),
            dma((n_r - 1,)),
            dma((n_r - 1,)),
            dma((2,)),
            dma((2,)),
            dma((1,)),
        ]
    gram, arrived = pl.pallas_call(
        functools.partial(folded_kernel if folded else kernel, n_r, n_s, math.sqrt(rows * n_r)),
        out_shape=(
            jax.ShapeDtypeStruct((n_s * width // n_r, width), f32),
            jax.ShapeDtypeStruct((rows, width), f32),
        ),
        in_specs=[hbm, vmem, hbm] if folded else [vmem, vmem, vmem],
        out_specs=(vmem, hbm),
        scratch_shapes=scratch,
        compiler_params=pltpu.CompilerParams(
            collective_id=0, has_side_effects=True, vmem_limit_bytes=62 * 1024 * 1024
        ),
    )(snapshots, weights.reshape(-1, 128), next_bricks)
    n_bricks = brick_source.shape[1]
    tiles, gram = pl.pallas_call(
        functools.partial(place_bricks, n_bricks),
        out_shape=(
            jax.ShapeDtypeStruct((rows, width), f32),
            jax.ShapeDtypeStruct(gram.shape, f32),
        ),
        in_specs=[pl.BlockSpec(memory_space=pltpu.SMEM), hbm, hbm],
        out_specs=(hbm, hbm),
        scratch_shapes=[
            pltpu.VMEM((rows, width), f32),
            pltpu.VMEM(gram.shape, f32),
            dma((n_bricks,)),
            dma((GROUPS,)),
            dma((2,)),
        ],
    )(brick_source, arrived, gram)
    return gram, tiles


def solution(mesh):
    placed = (P("rows", "snaps"), P("rows"), P(("rows", "snaps"), None), P("rows", None))
    return jax.shard_map(
        functools.partial(per_device, mesh.shape["rows"], mesh.shape["snaps"]),
        mesh=mesh,
        in_specs=placed,
        out_specs=(P("rows", "snaps"), P("rows", "snaps")),
        check_vma=False,
    )
```

```python
import functools
import math

import jax
import jax.numpy as jnp
from jax import lax
from jax.experimental import pallas as pl
from jax.experimental.pallas import tpu as pltpu
from jax.sharding import PartitionSpec as P

MESH = pl.DeviceIdType.MESH
STEP = 256
PIECES = 2
GROUPS = 8


def split(x):
    hi = x.astype(jnp.bfloat16)
    return hi, (x - hi.astype(jnp.float32)).astype(jnp.bfloat16)


def tdot(a, b):
    return lax.dot_general(a, b, (((0,), (0,)), ((), ())), preferred_element_type=jnp.float32)


def kernel(
    n_r, n_s, scale,
    snap, wts, bricks,
    gram, arrived,
    gbuf, mate, w_hi, w_lo, part, rs_buf, h_send, h_recv,
    ring_send, ring_recv, brick_send, brick_recv, rs_send, rs_recv, d_send, d_recv, own_sem,
):
    n = n_s // 2
    z = lax.axis_index("rows")
    s = lax.axis_index("snaps")
    c = s % 2
    chip = s // 2
    rows, width = snap.shape
    per_brick_dev = bricks.shape[0]

    def ring_of(i):
        u, v = i // 2, i % 2
        return u + v * (n - 1 - 2 * u)

    def chip_at(t):
        v = t // (n // 2)
        return 2 * (t + v * (n - 1 - 2 * t)) + v

    t = ring_of(chip)
    partner = chip * 2 + (1 - c)
    nxt = chip_at((t + 1) % n) * 2 + c
    prv = chip_at((t + n - 1) % n) * 2 + c

    barrier = pltpu.get_barrier_semaphore()
    for k in range(1, n_s):
        pl.semaphore_signal(barrier, inc=1, device_id=(z, (s + k) % n_s), device_id_type=MESH)
    for k in range(1, n_r):
        pl.semaphore_signal(barrier, inc=1, device_id=((z + k) % n_r, s), device_id_type=MESH)
    pl.semaphore_wait(barrier, n_s - 1 + n_r - 1)

    half = rows // 2
    piece = half // PIECES

    def ring_copy(way, hop, q):
        r0 = way * half + q * piece
        there = (n - hop if way == 0 else hop) - 1
        if hop == 1:
            src = snap.at[pl.ds(r0, piece)]
        else:
            here = (n - hop + 1 if way == 0 else hop - 1) - 1
            src = gbuf.at[here, pl.ds(r0, piece)]
        return pltpu.make_async_remote_copy(
            src_ref=src,
            dst_ref=gbuf.at[there, pl.ds(r0, piece)],
            send_sem=ring_send.at[way, hop - 1, q],
            recv_sem=ring_recv.at[way, hop - 1, q],
            device_id=(z, nxt if way == 0 else prv),
            device_id_type=MESH,
        )

    def brick_copy(k):
        to = (s + k) % n_s
        return pltpu.make_async_remote_copy(
            src_ref=bricks.at[:, pl.ds(pl.multiple_of(to * width, width), width)],
            dst_ref=arrived.at[pl.ds(pl.multiple_of(s * per_brick_dev, per_brick_dev), per_brick_dev)],
            send_sem=brick_send.at[k - 1],
            recv_sem=brick_recv.at[k - 1],
            device_id=(z, to),
            device_id_type=MESH,
        )

    def rs_copy(slot, k, home):
        return pltpu.make_async_remote_copy(
            src_ref=part.at[slot],
            dst_ref=rs_buf.at[k - 1],
            send_sem=rs_send.at[k - 1],
            recv_sem=rs_recv.at[k - 1],
            device_id=(home, s),
            device_id_type=MESH,
        )

    def d2d(i, src, dst):
        return pltpu.make_async_remote_copy(
            src_ref=src, dst_ref=dst, send_sem=d_send.at[i], recv_sem=d_recv.at[i],
            device_id=(z, partner), device_id_type=MESH,
        )

    for q in range(PIECES):
        for way in range(2):
            ring_copy(way, 1, q).start()
    own_bricks = pltpu.make_async_copy(
        bricks.at[:, pl.ds(pl.multiple_of(s * width, width), width)],
        arrived.at[pl.ds(pl.multiple_of(s * per_brick_dev, per_brick_dev), per_brick_dev)],
        own_sem.at[0],
    )
    own_bricks.start()
    to_mate = d2d(0, snap, mate)
    to_mate.start()

    def weigh(src, col):
        def body(i, carry):
            r0 = pl.multiple_of(i * 128, 128)
            w = jnp.broadcast_to(wts[pl.ds(i, 1), :], (128, 128)).T
            for l in range(width // 128):
                hi, lo = split(src[pl.ds(r0, 128), l * 128:(l + 1) * 128] * w)
                w_hi[pl.ds(r0, 128), col + l * 128:col + (l + 1) * 128] = hi
                w_lo[pl.ds(r0, 128), col + l * 128:col + (l + 1) * 128] = lo
            return carry
        lax.fori_loop(0, rows // 128, body, 0)

    def gather_product(slot, load, r0, count):
        def body(i, carry):
            r = pl.multiple_of(r0 + i * STEP, STEP)
            hi, lo = split(load(r))
            bh = w_hi[pl.ds(r, STEP), :]
            bl = w_lo[pl.ds(r, STEP), :]
            part[slot] += tdot(hi, bh) + (tdot(hi, bl) + tdot(lo, bh))
            return carry
        lax.fori_loop(0, count // STEP, body, 0)

    def send_home(slot):
        home = chip_at((t + slot) % n)
        k = (home + n_r - z) % n_r

        @pl.when(k > 0)
        def _():
            rs_copy(slot, k, home).start()

    weigh(snap, 0)
    part[...] = jnp.zeros_like(part)
    to_mate.wait()
    weigh(mate, width)
    gather_product(0, lambda r: snap[pl.ds(r, STEP), :], 0, rows)
    send_home(0)

    done = [0] * n
    for hop in range(1, n):
        for q in range(PIECES):
            for way in range(2):
                ring_copy(way, hop, q).wait_recv()
                if hop < n - 1:
                    ring_copy(way, hop + 1, q).start()
            if q == PIECES - 1 and hop == n - 2:
                for k in range(1, n_s):
                    brick_copy(k).start()
            for way in range(2):
                slot = n - hop if way == 0 else hop
                gather_product(
                    slot,
                    lambda r, slot=slot: gbuf[slot - 1, pl.ds(r, STEP), :],
                    way * half + q * piece,
                    piece,
                )
        for way in range(2):
            slot = n - hop if way == 0 else hop
            done[slot] += 1
            if done[slot] == 2:
                send_home(slot)

    for k in range(1, n_r):
        rs_copy(0, k, (z + k) % n_r).wait_recv()
    own = (ring_of(z) + n - t) % n
    total = part[own]
    for k in range(1, n_r):
        total += rs_buf[k - 1]
    total = total / scale
    h_send[...] = total[:, width:]
    to_other = d2d(1, h_send, h_recv)
    to_other.start()
    gram[pl.ds(pl.multiple_of(c * width, width), width), :] = total[:, :width]

    for k in range(1, n_s):
        brick_copy(k).wait_recv()
    own_bricks.wait()
    to_other.wait()
    gram[pl.ds(pl.multiple_of((1 - c) * width, width), width), :] = h_recv[...]
    for hop in range(1, n):
        for q in range(PIECES):
            for way in range(2):
                ring_copy(way, hop, q).wait_send()
    for k in range(1, n_s):
        brick_copy(k).wait_send()
    for k in range(1, n_r):
        rs_copy(0, k, (z + k) % n_r).wait_send()


def folded_kernel(
    n_r, n_s, scale,
    snap_in, wts, bricks,
    gram, arrived,
    snap, bounce, gbuf, mate, w_hi, w_lo, part, rs_buf, quad, xbuf, fin, fbuf,
    ring_send, ring_recv, brick_send, brick_recv, rs_send, rs_recv,
    x_send, x_recv, f_send, f_recv, d_send, d_recv, own_sem, in_sem,
):
    n = n_s // 2
    z = lax.axis_index("rows")
    s = lax.axis_index("snaps")
    c = s % 2
    chip = s // 2
    rows, width = snap_in.shape
    per_brick_dev = bricks.shape[0]

    def ring_of(i):
        u, v = i // 2, i % 2
        return u + v * (n - 1 - 2 * u)

    def chip_at(t):
        v = t // (n // 2)
        return 2 * (t + v * (n - 1 - 2 * t)) + v

    t = ring_of(chip)
    partner = chip * 2 + (1 - c)
    nxt = chip_at((t + 1) % n) * 2 + c
    prv = chip_at((t + n - 1) % n) * 2 + c

    load_snap = pltpu.make_async_copy(snap_in, snap, in_sem.at[0])
    load_snap.start()
    own_bricks_in = pltpu.make_async_copy(
        bricks.at[:, pl.ds(pl.multiple_of(s * width, width), width)], bounce, in_sem.at[1]
    )
    own_bricks_in.start()
    barrier = pltpu.get_barrier_semaphore()
    for k in range(1, n_s):
        pl.semaphore_signal(barrier, inc=1, device_id=(z, (s + k) % n_s), device_id_type=MESH)
    for k in range(1, n_r):
        for who in (s, partner):
            pl.semaphore_signal(barrier, inc=1, device_id=((z + k) % n_r, who), device_id_type=MESH)
    load_snap.wait()
    pl.semaphore_wait(barrier, n_s - 1 + 2 * (n_r - 1))

    half = rows // 2
    piece = half // 2

    def start_of(way, owner, other):
        q = owner // 2
        q = q + other * (1 - 2 * q)
        return pl.multiple_of(way * half + q * piece, piece)

    def slot_of(way):
        return n - 1 - way * (n - 2)

    def owner_of(way):
        return (t + n - 1 + 2 * way) % n

    def ring_copy(way, stage):
        if stage < 2:
            r0 = start_of(way, t, stage)
            src = snap.at[pl.ds(r0, piece)]
            there = n - 1 - way * (n - 2)
        else:
            owner = owner_of(way)
            r0 = start_of(way, owner, 0)
            src = gbuf.at[slot_of(way) - 1, pl.ds(r0, piece)]
            there = 2
        return pltpu.make_async_remote_copy(
            src_ref=src,
            dst_ref=gbuf.at[there - 1, pl.ds(r0, piece)],
            send_sem=ring_send.at[way, stage],
            recv_sem=ring_recv.at[way, stage],
            device_id=(z, nxt + way * (prv - nxt)),
            device_id_type=MESH,
        )

    def brick_copy(k):
        to = chip_at((t + k // 2) % n) * 2 + (c + k) % 2
        return pltpu.make_async_remote_copy(
            src_ref=bricks.at[:, pl.ds(pl.multiple_of(to * width, width), width)],
            dst_ref=arrived.at[pl.ds(pl.multiple_of(s * per_brick_dev, per_brick_dev), per_brick_dev)],
            send_sem=brick_send.at[k - 1],
            recv_sem=brick_recv.at[k - 1],
            device_id=(z, to),
            device_id_type=MESH,
        )

    def level_of(other, row_core, col_core):
        low = jnp.where(chip <= other, 1, 0)
        return low * (2 * row_core + col_core) + (1 - low) * (2 * col_core + row_core)

    def chunk(d):
        return chip_at((t + d) % n)

    def col_core_here(d):
        low = jnp.where(chip <= chunk(d), 1, 0)
        return low * (z % 2) + (1 - low) * (z // 2)

    def holds(d):
        low = jnp.where(chip <= chunk(d), 1, 0)
        return low * (z // 2) + (1 - low) * (z % 2) == c

    def rs_copy(d, side, k, home):
        return pltpu.make_async_remote_copy(
            src_ref=part.at[d, :, pl.ds(side * width, width)],
            dst_ref=rs_buf.at[d, k - 1],
            send_sem=rs_send.at[d, side],
            recv_sem=rs_recv.at[d, k - 1],
            device_id=(home, s),
            device_id_type=MESH,
        )

    def x_copy(d):
        return pltpu.make_async_remote_copy(
            src_ref=quad.at[d],
            dst_ref=xbuf.at[n - d - 1],
            send_sem=x_send.at[d - 1],
            recv_sem=x_recv.at[n - d - 1],
            device_id=(z, chunk(d) * 2 + col_core_here(d)),
            device_id_type=MESH,
        )

    def x_arrival(d):
        return pltpu.make_async_remote_copy(
            src_ref=quad.at[d],
            dst_ref=xbuf.at[d - 1],
            send_sem=x_send.at[d - 1],
            recv_sem=x_recv.at[d - 1],
            device_id=(z, chunk(d) * 2 + col_core_here(d)),
            device_id_type=MESH,
        )

    def f_copy(d):
        return pltpu.make_async_remote_copy(
            src_ref=fin.at[d],
            dst_ref=fbuf.at[c],
            send_sem=f_send.at[d],
            recv_sem=f_recv.at[c],
            device_id=(chunk(d), chip * 2 + col_core_here(d)),
            device_id_type=MESH,
        )

    def f_arrival(a):
        return pltpu.make_async_remote_copy(
            src_ref=fin.at[0],
            dst_ref=fbuf.at[a],
            send_sem=f_send.at[0],
            recv_sem=f_recv.at[a],
            device_id=((z + 1) % n_r, s),
            device_id_type=MESH,
        )

    first, second = c, 1 - c
    for stage in range(2):
        ring_copy(first, stage).start()
    own_bricks_in.wait()
    own_bricks = pltpu.make_async_copy(
        bounce,
        arrived.at[pl.ds(pl.multiple_of(s * per_brick_dev, per_brick_dev), per_brick_dev)],
        own_sem.at[0],
    )
    own_bricks.start()
    brick_copy(1).start()
    to_mate = pltpu.make_async_remote_copy(
        src_ref=snap, dst_ref=mate, send_sem=d_send.at[0], recv_sem=d_recv.at[0],
        device_id=(z, partner), device_id_type=MESH,
    )
    to_mate.start()

    def weigh(src, col):
        def body(i, carry):
            r0 = pl.multiple_of(i * 128, 128)
            w = jnp.broadcast_to(wts[pl.ds(i, 1), :], (128, 128)).T
            for l in range(width // 128):
                hi, lo = split(src[pl.ds(r0, 128), l * 128:(l + 1) * 128] * w)
                w_hi[pl.ds(r0, 128), col + l * 128:col + (l + 1) * 128] = hi
                w_lo[pl.ds(r0, 128), col + l * 128:col + (l + 1) * 128] = lo
            return carry
        lax.fori_loop(0, rows // 128, body, 0)

    def gather_product(slot, load, r0, count):
        def body(i, carry):
            r = pl.multiple_of(r0 + i * STEP, STEP)
            hi, lo = split(load(r))
            bh = w_hi[pl.ds(r, STEP), :]
            bl = w_lo[pl.ds(r, STEP), :]
            part[slot] += tdot(hi, bh) + (tdot(hi, bl) + tdot(lo, bh))
            return carry
        lax.fori_loop(0, count // STEP, body, 0)

    def take(slot, r0):
        gather_product(slot, lambda r: gbuf[slot - 1, pl.ds(r, STEP), :], r0, piece)

    def sides(d, act):
        for side in range(2):
            home = level_of(chunk(d), c, (c + side) % 2)
            k = (home + n_r - z) % n_r

            @pl.when(k > 0)
            def _():
                act(rs_copy(d, side, k, home))

    weigh(snap, 0)
    part[...] = jnp.zeros_like(part)
    to_mate.wait()
    weigh(mate, width)
    gather_product(0, lambda r: snap[pl.ds(r, STEP), :], 0, rows)
    sides(0, lambda copy: copy.start())

    def finish(d):
        col_core = col_core_here(d)
        home = chunk(d)
        here = jnp.where(home == z, 1, 0) * jnp.where(col_core == c, 1, 0)

        @pl.when(here == 0)
        def _():
            f_copy(d).start()

        @pl.when(here == 1)
        def _():
            fbuf[c] = fin[d]

    def reduce_quadrant(d):
        @pl.when(holds(d))
        def _():
            for k in range(1, n_r):
                rs_copy(d, 0, k, (z + k) % n_r).wait_recv()
            side = (col_core_here(d) + c) % 2
            total = part[d, :, pl.ds(pl.multiple_of(side * width, width), width)]
            for k in range(1, n_r):
                total += rs_buf[d, k - 1]
            if d == 0:
                fin[0] = total / scale
                finish(0)
            else:
                quad[d] = total
                x_copy(d).start()
    def near(way):
        for stage in range(2):
            ring_copy(way, stage).wait_recv()
        slot = slot_of(way)
        for stage in range(2):
            take(slot, start_of(way, owner_of(way), stage))
        sides(slot, lambda copy: copy.start())

    for stage in range(2):
        ring_copy(first, stage).wait_send()
        ring_copy(second, stage).start()
    near(first)
    for stage in range(2):
        ring_copy(second, stage).wait_send()
        if stage == 0:
            ring_copy(first, 2).start()
    ring_copy(second, 0).wait_recv()
    ring_copy(second, 2).start()
    reduce_quadrant(0)
    ring_copy(second, 1).wait_recv()
    for stage in range(2):
        take(slot_of(second), start_of(second, owner_of(second), stage))
    sides(slot_of(second), lambda copy: copy.start())
    for way in range(2):
        ring_copy(way, 2).wait_recv()
        take(2, start_of(way, (t + 2) % n, 0))
    sides(2, lambda copy: copy.start())
    for k in (4, 5):
        brick_copy(k).start()

    order = (1, 3, 2)
    for d in order:
        reduce_quadrant(d)
    for k in (2, 3, 6, 7):
        brick_copy(k).start()
    for d in order:
        @pl.when(holds(d))
        def _():
            x_arrival(d).wait_recv()
            fin[d] = (quad[d] + xbuf[d - 1].T) / scale
            finish(d)

    for k in range(1, n_s):
        brick_copy(k).wait_recv()
    own_bricks.wait()
    for a in range(2):
        level = level_of(z, a, c)
        same = jnp.where(level == z, 1, 0) * jnp.where(c == a, 1, 0)

        @pl.when(same == 0)
        def _():
            f_arrival(a).wait_recv()

        gram[a * width:(a + 1) * width, :] = fbuf[a]

    for way in range(2):
        ring_copy(way, 2).wait_send()
    for k in range(1, n_s):
        brick_copy(k).wait_send()
    for d in range(n):
        sides(d, lambda copy: copy.wait_send())

        @pl.when(holds(d))
        def _():
            if d > 0:
                x_copy(d).wait_send()
            here = jnp.where(chunk(d) == z, 1, 0) * jnp.where(col_core_here(d) == c, 1, 0)

            @pl.when(here == 0)
            def _():
                f_copy(d).wait_send()


def place_bricks(n_bricks, order, src, gram, dst, gram_out, buf, gram_buf, in_sem, out_sem, g_sem):
    gram_in = pltpu.make_async_copy(gram, gram_buf, g_sem.at[0])
    gram_in.start()
    tall = src.shape[0] // n_bricks
    group = n_bricks // GROUPS

    def fetch(i):
        return pltpu.make_async_copy(
            src.at[pl.ds(pl.multiple_of(order[0, i] * tall, tall), tall)],
            buf.at[pl.ds(pl.multiple_of(i * tall, tall), tall)],
            in_sem.at[i],
        )

    def put(g):
        block = pl.ds(g * group * tall, group * tall)
        return pltpu.make_async_copy(buf.at[block], dst.at[block], out_sem.at[g])

    def start(i, carry):
        fetch(i).start()
        return carry

    def wait(i, carry):
        fetch(i).wait()
        return carry

    lax.fori_loop(0, n_bricks, start, 0)
    for g in range(GROUPS):
        lax.fori_loop(g * group, (g + 1) * group, wait, 0)
        put(g).start()
    gram_in.wait()
    gram_put = pltpu.make_async_copy(gram_buf, gram_out, g_sem.at[1])
    gram_put.start()
    for g in range(GROUPS):
        put(g).wait()
    gram_put.wait()


def per_device(n_r, n_s, snapshots, weights, next_bricks, brick_source):
    rows, width = snapshots.shape
    n = n_s // 2
    assert n == n_r and n % 2 == 0
    f32, bf16 = jnp.float32, jnp.bfloat16
    vmem = pl.BlockSpec(memory_space=pltpu.VMEM)
    dma = pltpu.SemaphoreType.DMA
    wide = 2 * width
    hbm = pl.BlockSpec(memory_space=pl.ANY)
    scratch = [
        pltpu.VMEM((n - 1, rows, width), f32),
        pltpu.VMEM((rows, width), f32),
        pltpu.VMEM((rows, wide), bf16),
        pltpu.VMEM((rows, wide), bf16),
        pltpu.VMEM((n, width, wide), f32),
    ]
    folded = n == 4
    if folded:
        scratch = [pltpu.VMEM((rows, width), f32), pltpu.VMEM((rows // n_s, width), f32)] + scratch + [
            pltpu.VMEM((n, n_r - 1, width, width), f32),
            pltpu.VMEM((n, width, width), f32),
            pltpu.VMEM((n - 1, width, width), f32),
            pltpu.VMEM((n, width, width), f32),
            pltpu.VMEM((2, width, width), f32),
            dma((2, 3)),
            dma((2, 3)),
            dma((n_s - 1,)),
            dma((n_s - 1,)),
            dma((n, 2)),
            dma((n, n_r - 1)),
            dma((n - 1,)),
            dma((n - 1,)),
            dma((n,)),
            dma((2,)),
            dma((1,)),
            dma((1,)),
            dma((1,)),
            dma((2,)),
        ]
    else:
        scratch += [
            pltpu.VMEM((n_r - 1, width, wide), f32),
            pltpu.VMEM((width, width), f32),
            pltpu.VMEM((width, width), f32),
            dma((2, n - 1, PIECES)),
            dma((2, n - 1, PIECES)),
            dma((n_s - 1,)),
            dma((n_s - 1,)),
            dma((n_r - 1,)),
            dma((n_r - 1,)),
            dma((2,)),
            dma((2,)),
            dma((1,)),
        ]
    gram, arrived = pl.pallas_call(
        functools.partial(folded_kernel if folded else kernel, n_r, n_s, math.sqrt(rows * n_r)),
        out_shape=(
            jax.ShapeDtypeStruct((n_s * width // n_r, width), f32),
            jax.ShapeDtypeStruct((rows, width), f32),
        ),
        in_specs=[hbm, vmem, hbm] if folded else [vmem, vmem, vmem],
        out_specs=(vmem, hbm),
        scratch_shapes=scratch,
        compiler_params=pltpu.CompilerParams(
            collective_id=0, has_side_effects=True, vmem_limit_bytes=62 * 1024 * 1024
        ),
    )(snapshots, weights.reshape(-1, 128), next_bricks)
    n_bricks = brick_source.shape[1]
    tiles, gram = pl.pallas_call(
        functools.partial(place_bricks, n_bricks),
        out_shape=(
            jax.ShapeDtypeStruct((rows, width), f32),
            jax.ShapeDtypeStruct(gram.shape, f32),
        ),
        in_specs=[pl.BlockSpec(memory_space=pltpu.SMEM), hbm, hbm],
        out_specs=(hbm, hbm),
        scratch_shapes=[
            pltpu.VMEM((rows, width), f32),
            pltpu.VMEM(gram.shape, f32),
            dma((n_bricks,)),
            dma((GROUPS,)),
            dma((2,)),
        ],
    )(brick_source, arrived, gram)
    return gram, tiles


def solution(mesh):
    placed = (P("rows", "snaps"), P("rows"), P(("rows", "snaps"), None), P("rows", None))
    return jax.shard_map(
        functools.partial(per_device, mesh.shape["rows"], mesh.shape["snaps"]),
        mesh=mesh,
        in_specs=placed,
        out_specs=(P("rows", "snaps"), P("rows", "snaps")),
        check_vma=False,
    )
```
